32 devices in a mesh: slab: 8 (over y, x, core), tm: 4 (over z).
Axes of the slice: x: 2, y: 2, z: 4, core: 2. Of those that a mesh axis runs over, the one named last changes fastest.
Arguments:
- field: float32 [2, 128, 256, 512], P(None, 'slab', None, 'tm'), may hold values from -110 to 110
Outputs:
- evolved: float32 [2, 128, 256, 512], P(None, 'slab', None, 'tm')
The draws below stay inside these ranges and needn't reach their ends.
All inputs are finite; a program needn't handle non-finite values.
Results may differ from the reference program's by a relative error of at most 0.000098.
Values sent between devices are 32-bit elements; how exact they have to be, the bound alone decides.
A program may use at most 128 MiB of HBM per device.

```python
import math
import jax
import jax.numpy as jnp
from jax import lax

NX = 128
NY = 256
NT = 512


def draw_field(key, part):
    key_rows = jax.random.fold_in(key, 11)
    key_times = jax.random.fold_in(key, 23)
    key_entries = jax.random.fold_in(key, 37)
    log_ten = math.log(10.0)
    rising = 1.0 + 2.0 * jnp.arange(NX, dtype=jnp.float32) / NX
    row_scale = jnp.exp(jax.random.uniform(key_rows, (NX,), jnp.float32, 0.0, log_ten)) * rising
    time_scale = jnp.exp(jax.random.uniform(key_times, (NT,), jnp.float32, 0.0, log_ten))
    entries = jnp.clip(jax.random.normal(key_entries, (2, NX, NY, NT), jnp.float32), -6.0, 6.0)
    amplitude = jnp.sqrt(row_scale[:, None, None] * time_scale[None, None, :])
    return entries * amplitude[None]


def setup_inputs(seed: int = 0) -> dict:
    arg_keys = jax.random.split(jax.random.key(seed), 2)
    field = draw_field(jax.random.fold_in(arg_keys[1], 71), 0)
    return dict(field=field)


TWO_PI = 2.0 * math.pi
DIFFRACT = 4.0
DISPERSE = 3.0
KERR = 0.05
WELL = 1.5
EPSILON = 1e-06

def frequency(length):
    positions = jnp.arange(length, dtype=jnp.int32)
    signed = jnp.where(2 * positions < length, positions, positions - length)
    return signed.astype(jnp.float32) * (TWO_PI / length)

def reference(field):
    mean_power = jnp.mean(field[0] * field[0] + field[1] * field[1])
    launch_scale = 1.0 / jnp.sqrt(mean_power + EPSILON)
    launched = lax.complex(field[0] * launch_scale, field[1] * launch_scale)
    across_x = frequency(NX)
    across_y = frequency(NY)
    temporal = frequency(NT)
    theta = -DIFFRACT * (across_x[:, None, None] ** 2 + across_y[None, :, None] ** 2) + DISPERSE * temporal[None, None, :] ** 2
    rotor = lax.complex(jnp.cos(theta), jnp.sin(theta))

    def half_step(wave):
        return jnp.fft.ifftn(jnp.fft.fftn(wave, axes=(0, 1, 2)) * rotor, axes=(0, 1, 2))
    after_half = half_step(launched)
    place_x = (jnp.arange(NX, dtype=jnp.float32) - (NX - 1) / 2.0) / (NX / 2.0)
    place_y = (jnp.arange(NY, dtype=jnp.float32) - (NY - 1) / 2.0) / (NY / 2.0)
    well_depth = WELL * (place_x[:, None, None] ** 2 + place_y[None, :, None] ** 2)
    intensity = jnp.real(after_half) ** 2 + jnp.imag(after_half) ** 2
    kick_angle = KERR * intensity - well_depth
    kicked = after_half * lax.complex(jnp.cos(kick_angle), jnp.sin(kick_angle))
    evolved = half_step(kicked)
    return jnp.stack([jnp.real(evolved), jnp.imag(evolved)])
```

```python
import math

import numpy as np

import jax
import jax.numpy as jnp
from jax import lax
from jax.sharding import PartitionSpec as P

TWO_PI = 2.0 * math.pi
DIFFRACT = 4.0
DISPERSE = 3.0
KERR = 0.05
WELL = 1.5
EPSILON = 1e-06
AXES = ("slab", "tm")
CHUNKS = 2


def propagator(length, strength):
    steps = np.arange(length)
    signed = np.where(2 * steps < length, steps, steps - length)
    phase = np.exp(1j * strength * (TWO_PI * signed / length) ** 2)
    response = np.fft.ifft(phase)
    matrix = response[(steps[:, None] - steps[None, :]) % length]
    real = jnp.asarray(matrix.real.astype(np.float32))
    imag = jnp.asarray(matrix.imag.astype(np.float32))
    upper = jnp.stack([real, -imag], axis=1)
    lower = jnp.stack([imag, real], axis=1)
    return jnp.stack([upper, lower])


def apply(form, table, value):
    return jnp.einsum(form, table, value, precision=lax.Precision.HIGH)


def place(index, length):
    return (index.astype(jnp.float32) - (length - 1) / 2.0) / (length / 2.0)


def kick(real, imag, scale, well_depth):
    real = real * scale
    imag = imag * scale
    angle = KERR * (real * real + imag * imag) - well_depth
    turn_c = jnp.cos(angle)
    turn_s = jnp.sin(angle)
    return real * turn_c - imag * turn_s, real * turn_s + imag * turn_c


def on_device(field):
    slabs = lax.axis_size("slab")
    times = lax.axis_size("tm")
    devices = slabs * times
    _, rows, ny, cols = field.shape
    nx = rows * slabs
    nt = cols * times
    along_x = propagator(nx, -DIFFRACT)
    along_y = propagator(ny, -DIFFRACT)
    along_t = propagator(nt, DISPERSE)
    partial_power = jnp.sum(field[0] * field[0] + field[1] * field[1])
    mean_power = lax.psum(partial_power, AXES) / (nx * ny * nt)
    scale = 1.0 / jnp.sqrt(mean_power + EPSILON)
    index_x = jnp.arange(nx, dtype=jnp.int32)

    if ny % devices == 0:
        group = ny // devices
        chunks = math.gcd(group, CHUNKS)
        piece = group // chunks
        spread = along_y.reshape(2, devices, chunks, piece, 2, ny)
        gather = along_y.reshape(2, ny, 2, devices, chunks, piece)
        arrived = []
        for chunk in range(chunks):
            table = spread[:, :, chunk].reshape(2, devices * piece, 2, ny)
            sent = apply("qzpb,pabc->zqac", table, field)
            if chunk == 1:
                sent, scale = lax.optimization_barrier((sent, scale))
            arrived.append(
                lax.all_to_all(sent, AXES, split_axis=0, concat_axis=0, tiled=True)
            )
        total = None
        for chunk in range(chunks):
            got = arrived[chunk].reshape(slabs, times, piece, 2, rows, cols)
            mixed = apply("qxpsa,smgpac->gqxmc", along_x.reshape(2, nx, 2, slabs, rows), got)
            whole = apply("rtqT,gqxT->grxt", along_t, mixed.reshape(piece, 2, nx, nt))
            first = lax.axis_index(AXES) * group + chunk * piece
            place_y = place(first + jnp.arange(piece, dtype=jnp.int32), ny)
            well_depth = WELL * (
                place(index_x, nx)[None, :, None] ** 2 + place_y[:, None, None] ** 2
            )
            kicked = jnp.stack(kick(whole[:, 0], whole[:, 1], scale, well_depth), axis=1)
            timed = apply("rtqT,gqxT->grxt", along_t, kicked)
            back = apply(
                "qsapX,gpXmc->smgqac",
                along_x.reshape(2, slabs, rows, 2, nx),
                timed.reshape(piece, 2, nx, times, cols),
            )
            home = lax.all_to_all(
                back.reshape(devices * piece, 2, rows, cols),
                AXES,
                split_axis=0,
                concat_axis=0,
                tiled=True,
            )
            table = gather[:, :, :, :, chunk].reshape(2, ny, 2, devices * piece)
            part = apply("qzpb,bpac->qazc", table, home)
            total = part if total is None else total + part
        return total

    group = ny // times
    width = group * nt // slabs
    sent = apply("qzpb,pabc->qazc", along_y, field)
    timed = lax.all_to_all(sent, "tm", split_axis=2, concat_axis=3, tiled=True)
    timed = apply("rtqT,qabT->rabt", along_t, timed)
    crossed = lax.all_to_all(
        timed.reshape(2, rows, slabs, width), "slab", split_axis=2, concat_axis=1, tiled=True
    ).reshape(2, nx, width)
    crossed = apply("qxpX,pXw->qxw", along_x, crossed)
    flat = lax.axis_index("slab") * width + jnp.arange(width, dtype=jnp.int32)
    place_y = place(lax.axis_index("tm") * group + flat // nt, ny)
    well_depth = WELL * (place(index_x, nx)[:, None] ** 2 + place_y[None, :] ** 2)
    kicked = jnp.stack(kick(crossed[0], crossed[1], scale, well_depth))
    kicked = apply("qxpX,pXw->qxw", along_x, kicked)
    timed = lax.all_to_all(
        kicked.reshape(2, nx, 1, width), "slab", split_axis=1, concat_axis=2, tiled=True
    ).reshape(2, rows, group, nt)
    timed = apply("rtqT,qabT->rabt", along_t, timed)
    home = lax.all_to_all(timed, "tm", split_axis=3, concat_axis=2, tiled=True)
    return apply("qzpb,pabc->qazc", along_y, home)


def solution(mesh):
    placed = (P(None, "slab", None, "tm"),)
    return jax.shard_map(
        on_device,
        mesh=mesh,
        in_specs=placed,
        out_specs=P(None, "slab", None, "tm"),
        check_vma=False,
    )
```

```python
import math

import numpy as np

import jax
import jax.numpy as jnp
from jax import lax
from jax.sharding import PartitionSpec as P

TWO_PI = 2.0 * math.pi
DIFFRACT = 4.0
DISPERSE = 3.0
KERR = 0.05
WELL = 1.5
EPSILON = 1e-06
AXES = ("slab", "tm")
CHUNKS = 2


def propagator(length, strength):
    steps = np.arange(length)
    signed = np.where(2 * steps < length, steps, steps - length)
    phase = np.exp(1j * strength * (TWO_PI * signed / length) ** 2)
    response = np.fft.ifft(phase)
    matrix = response[(steps[:, None] - steps[None, :]) % length]
    real = jnp.asarray(matrix.real.astype(np.float32))
    imag = jnp.asarray(matrix.imag.astype(np.float32))
    upper = jnp.stack([real, -imag], axis=1)
    lower = jnp.stack([imag, real], axis=1)
    return jnp.stack([upper, lower])


def apply(form, table, value):
    return jnp.einsum(form, table, value, precision=lax.Precision.HIGH)


def place(index, length):
    return (index.astype(jnp.float32) - (length - 1) / 2.0) / (length / 2.0)


def kick(real, imag, scale, well_depth):
    real = real * scale
    imag = imag * scale
    angle = KERR * (real * real + imag * imag) - well_depth
    turn_c = jnp.cos(angle)
    turn_s = jnp.sin(angle)
    return real * turn_c - imag * turn_s, real * turn_s + imag * turn_c


def on_device(field):
    slabs = lax.axis_size("slab")
    times = lax.axis_size("tm")
    devices = slabs * times
    _, rows, ny, cols = field.shape
    nx = rows * slabs
    nt = cols * times
    along_x = propagator(nx, -DIFFRACT)
    along_y = propagator(ny, -DIFFRACT)
    along_t = propagator(nt, DISPERSE)
    partial_power = jnp.sum(field[0] * field[0] + field[1] * field[1])
    powers = lax.all_to_all(
        jnp.broadcast_to(partial_power, (devices, 128)), AXES, split_axis=0, concat_axis=0, tiled=True
    )
    mean_power = jnp.sum(powers[:, 0]) / (nx * ny * nt)
    scale = 1.0 / jnp.sqrt(mean_power + EPSILON)
    index_x = jnp.arange(nx, dtype=jnp.int32)

    if ny % devices == 0:
        group = ny // devices
        chunks = math.gcd(group, CHUNKS)
        piece = group // chunks
        spread = along_y.reshape(2, devices, chunks, piece, 2, ny)
        gather = along_y.reshape(2, ny, 2, devices, chunks, piece)
        arrived = []
        for chunk in range(chunks):
            table = spread[:, :, chunk].reshape(2, devices * piece, 2, ny)
            sent = apply("qzpb,pabc->zqac", table, field)
            arrived.append(
                lax.all_to_all(sent, AXES, split_axis=0, concat_axis=0, tiled=True)
            )
        total = None
        for chunk in range(chunks):
            got = arrived[chunk].reshape(slabs, times, piece, 2, rows, cols)
            mixed = apply("qxpsa,smgpac->gqxmc", along_x.reshape(2, nx, 2, slabs, rows), got)
            whole = apply("rtqT,gqxT->grxt", along_t, mixed.reshape(piece, 2, nx, nt))
            first = lax.axis_index(AXES) * group + chunk * piece
            place_y = place(first + jnp.arange(piece, dtype=jnp.int32), ny)
            well_depth = WELL * (
                place(index_x, nx)[None, :, None] ** 2 + place_y[:, None, None] ** 2
            )
            kicked = jnp.stack(kick(whole[:, 0], whole[:, 1], scale, well_depth), axis=1)
            timed = apply("rtqT,gqxT->grxt", along_t, kicked)
            back = apply(
                "qsapX,gpXmc->smgqac",
                along_x.reshape(2, slabs, rows, 2, nx),
                timed.reshape(piece, 2, nx, times, cols),
            )
            home = lax.all_to_all(
                back.reshape(devices * piece, 2, rows, cols),
                AXES,
                split_axis=0,
                concat_axis=0,
                tiled=True,
            )
            table = gather[:, :, :, :, chunk].reshape(2, ny, 2, devices * piece)
            part = apply("qzpb,bpac->qazc", table, home)
            total = part if total is None else total + part
        return total

    group = ny // times
    width = group * nt // slabs
    sent = apply("qzpb,pabc->qazc", along_y, field)
    timed = lax.all_to_all(sent, "tm", split_axis=2, concat_axis=3, tiled=True)
    timed = apply("rtqT,qabT->rabt", along_t, timed)
    crossed = lax.all_to_all(
        timed.reshape(2, rows, slabs, width), "slab", split_axis=2, concat_axis=1, tiled=True
    ).reshape(2, nx, width)
    crossed = apply("qxpX,pXw->qxw", along_x, crossed)
    flat = lax.axis_index("slab") * width + jnp.arange(width, dtype=jnp.int32)
    place_y = place(lax.axis_index("tm") * group + flat // nt, ny)
    well_depth = WELL * (place(index_x, nx)[:, None] ** 2 + place_y[None, :] ** 2)
    kicked = jnp.stack(kick(crossed[0], crossed[1], scale, well_depth))
    kicked = apply("qxpX,pXw->qxw", along_x, kicked)
    timed = lax.all_to_all(
        kicked.reshape(2, nx, 1, width), "slab", split_axis=1, concat_axis=2, tiled=True
    ).reshape(2, rows, group, nt)
    timed = apply("rtqT,qabT->rabt", along_t, timed)
    home = lax.all_to_all(timed, "tm", split_axis=3, concat_axis=2, tiled=True)
    return apply("qzpb,pabc->qazc", along_y, home)


def solution(mesh):
    placed = (P(None, "slab", None, "tm"),)
    return jax.shard_map(
        on_device,
        mesh=mesh,
        in_specs=placed,
        out_specs=P(None, "slab", None, "tm"),
        check_vma=False,
    )
```
